32 devices in a mesh: kpt: 16 (over z, y, x), aux: 2 (over core).
Axes of the slice: x: 2, y: 2, z: 4, core: 2. Of those that a mesh axis runs over, the one named last changes fastest.
Arguments:
- pair_tensors: bfloat16 [2, 32, 4, 512, 1024], P(None, 'kpt', 'aux'), may hold values from -0.1875 to 0.1875
- orbitals: bfloat16 [32, 512, 512], P('kpt'), may hold values from -6 to 6
- matchings: int32 [2, 32], replicated, may hold values from 0 to 31, as said below
Outputs:
- exchange: float32 [32, 2, 512, 512], P('kpt', None, 'aux')
The draws below stay inside these ranges and needn't reach their ends.
Inputs may be any that keep to these rules, and one draw needn't show every extreme that they name: Each row matchings[r] is a permutation of the 32 k-points. With 2^m = 16 blocks of 2 consecutive k-points, round r matches every k-point of block d with a k-point of block d XOR 2^(m - 1 - r).
All inputs are finite; a program needn't handle non-finite values.
Results may differ from the reference program's by a relative error of at most 0.00098.
Values may be sent and summed in bfloat16 or wider, within the bound.
No kernel may reach another device: no remote copies, remote signals or barrier semaphores. Data moves between devices by JAX's collectives and lax.ppermute only.
A program may use at most 192 MiB of HBM per device.

```python
import jax
import jax.numpy as jnp
from jax import lax

NAO = 512
NOCC = 256
KPT_DEV = 2
ROUNDS = 2
KPTS = 32
NAUX = 4


def draw_matchings(key, part):
    blocks_count = KPTS // KPT_DEV
    bit_count = blocks_count.bit_length() - 1
    scores = jax.random.randint(key, (ROUNDS, blocks_count, KPT_DEV), 0, 2 ** 20, dtype=jnp.int32)
    scores = scores * KPT_DEV + jnp.arange(KPT_DEV, dtype=jnp.int32)
    within = jnp.argsort(scores, axis=-1, stable=True).astype(jnp.int32)
    block_ids = jnp.arange(blocks_count, dtype=jnp.int32)
    rows_out = []
    for which_round in range(ROUNDS):
        partner_block = jnp.bitwise_xor(block_ids, 1 << bit_count - 1 - which_round)
        matched = partner_block[:, None] * KPT_DEV + within[which_round]
        rows_out.append(matched.reshape(-1))
    return jnp.stack(rows_out, axis=0).astype(jnp.int32)


def level_of(rng, shape, cuts, smallest, largest):
    gain, own = 1.0, jax.random.fold_in(rng, 6)
    for axis_at, shards_of in cuts:
        draws = jnp.exp(jax.random.uniform(jax.random.fold_in(own, axis_at), (shards_of,), jnp.float32, smallest / len(cuts), largest / len(cuts)))
        gain = gain * jnp.repeat(draws, shape[axis_at] // shards_of).reshape([-1 if axis == axis_at else 1 for axis in range(len(shape))])
    return gain


def normal_values(own_key, shape, deviation, most, cuts=(), held_as=jnp.bfloat16):
    result = deviation * jax.random.normal(own_key, shape, jnp.float32)
    if cuts:
        result = result * level_of(own_key, shape, cuts, -0.22, 0.18)
    return jnp.clip(result, -most, most).astype(held_as)


def setup_inputs(seed: int = 0) -> dict:
    seeds = jax.random.split(jax.random.key(seed), 4)
    return {
        "pair_tensors": normal_values(seeds[0], (ROUNDS, KPTS, NAUX, NAO, 2 * NAO), (2 * NAO) ** -0.5, 0.1875, ((1, 16), (2, 2))),
        "orbitals": normal_values(seeds[1], (KPTS, NAO, 2 * NOCC), 1.0, 6.0, ((0, 16),)),
        "matchings": draw_matchings(jax.random.fold_in(seeds[3], 71), 0),
    }


def build_block(chosen):
    occupied = chosen.shape[-1] // 2
    real_part = chosen[..., :occupied]
    imag_part = chosen[..., occupied:]
    upper_rows = jnp.concatenate([real_part, imag_part], axis=-1)
    bottom = jnp.concatenate([-imag_part, real_part], axis=-1)
    return jnp.concatenate([upper_rows, bottom], axis=-2)


def reference(pair_tensors, orbitals, matchings):
    factor = 1.0 / (ROUNDS * NAUX * NOCC) ** 0.5
    high = lax.Precision.HIGHEST

    def one_point(index):
        running = jnp.zeros((2, NAO, NAO), jnp.float32)
        for which_round in range(ROUNDS):
            partner_id = matchings[which_round, index]
            chosen = lax.dynamic_index_in_dim(orbitals, partner_id, 0, keepdims=False)
            block = build_block(chosen).astype(jnp.float32)
            pairs = pair_tensors[which_round, index].astype(jnp.float32)
            half_done = jnp.einsum("pab,bc->pac", pairs, block, precision=high).astype(jnp.bfloat16)
            wide_half = half_done.astype(jnp.float32)
            real_half = wide_half[..., :NOCC]
            imag_half = wide_half[..., NOCC:]
            rotated = jnp.concatenate([-imag_half, real_half], axis=-1)
            exch_real = jnp.einsum("pac,pbc->ab", wide_half, wide_half, precision=high)
            exch_imag = jnp.einsum("pac,pbc->ab", wide_half, rotated, precision=high)
            running = running + jnp.stack([exch_real, exch_imag], axis=0) * factor
        return running

    return lax.map(one_point, jnp.arange(KPTS, dtype=jnp.int32))
```

```python
import functools

import jax
import jax.numpy as jnp
from jax import lax
from jax.experimental import pallas as pl
from jax.experimental.pallas import tpu as pltpu
from jax.sharding import PartitionSpec as P


ROUNDS = 2
VMEM_LIMIT = 24 << 20


def from_partner(shard, axis, distance):
    return lax.ppermute(shard, axis, [(i, i ^ 1 << distance) for i in range(lax.axis_size(axis))])


def from_sibling(shard):
    return lax.ppermute(shard, "aux", [(0, 1), (1, 0)])


def hop_round(index, blocks, wave):
    top = index // (blocks // 4)
    return (top + top // 2 + wave + 1) % 2


def wave_targets(blocks, wave):
    bit_count = blocks.bit_length() - 1
    pairs = []
    for index in range(blocks):
        for which_round in range(ROUNDS):
            partner = index ^ 1 << (bit_count - 1 - which_round)
            if hop_round(partner, blocks, wave) == which_round:
                pairs.append((index, partner))
    return pairs


def term_kernel(users, own_ref, sib_ref, mine_ref, other_ref, *rest, factor, wave, start, blocks):
    if wave or start:
        _, *rest = rest
    out_ref, pair_buf, block_ref, half_ref, left_ref, total_ref, pair_sems, prev_sem, out_sem = rest
    rows, width = mine_ref.shape[1:]
    funcs, nao = own_ref.shape[2:4]
    occupied = width // 2
    core = lax.axis_index("aux")
    which_round = hop_round(lax.axis_index("kpt"), blocks, wave)
    spot = users[which_round, start]
    loads = []
    for which, pair_ref in enumerate((own_ref, sib_ref)):
        for p in range(funcs):
            q = which * funcs + p
            loads.append(
                pltpu.make_async_copy(
                    pair_ref.at[which_round, spot, p], pair_buf.at[q], pair_sems.at[q]
                )
            )
    for load in loads:
        load.start()
    if wave:
        back = pltpu.make_async_copy(out_ref.at[spot], total_ref, prev_sem)
        back.start()
    for share, at in ((mine_ref, core), (other_ref, 1 - core)):
        value = share[0]
        top = pl.multiple_of(at * rows, rows)
        block_ref[pl.ds(top, rows), :] = value
        low = pl.multiple_of(nao + at * rows, rows)
        block_ref[pl.ds(low, rows), :occupied] = -value[:, occupied:]
        block_ref[pl.ds(low, rows), occupied:] = value[:, :occupied]
    mine_at = pl.multiple_of(core * rows, rows)
    for q in range(2 * funcs):
        loads[q].wait()
        half = jnp.dot(pair_buf[q], block_ref[...], preferred_element_type=jnp.float32)
        half_ref[q] = half.astype(jnp.bfloat16)
        left = half_ref[q, pl.ds(mine_at, rows), :]
        left_ref[q, :rows, :] = left
        left_ref[q, rows:, :occupied] = left[:, occupied:]
        left_ref[q, rows:, occupied:] = -left[:, :occupied]
    total = None
    for q in range(2 * funcs):
        part = lax.dot_general(
            left_ref[q], half_ref[q], (((1,), (1,)), ((), ())), preferred_element_type=jnp.float32
        )
        total = part if total is None else total + part
    total = (total * factor).reshape(2, rows, nao)
    if wave:
        back.wait()
        total = total_ref[...] + total
    total_ref[...] = total
    store = pltpu.make_async_copy(total_ref, out_ref.at[spot], out_sem)
    store.start()
    store.wait()


def add_terms(users, own, sib, mine, other, prev, factor, wave, start, blocks):
    rows, width = mine.shape[1:]
    per_device, funcs, nao = own.shape[1:4]
    vmem = pl.BlockSpec(memory_space=pltpu.VMEM)
    hbm = pl.BlockSpec(memory_space=pltpu.HBM)
    operands = [users, own, sib, mine, other]
    in_specs = [pl.BlockSpec(memory_space=pltpu.SMEM), hbm, hbm, vmem, vmem]
    aliases = {}
    if prev is not None:
        aliases = {len(operands): 0}
        operands.append(prev)
        in_specs.append(hbm)
    flops = funcs * 2 * (2 * nao * 2 * nao * width + 2 * 2 * rows * nao * width)
    kernel = functools.partial(term_kernel, factor=factor, wave=wave, start=start, blocks=blocks)
    return pl.pallas_call(
        kernel,
        out_shape=jax.ShapeDtypeStruct((per_device, 2, rows, nao), jnp.float32),
        in_specs=in_specs,
        out_specs=hbm,
        scratch_shapes=[
            pltpu.VMEM((2 * funcs, nao, 2 * nao), jnp.bfloat16),
            pltpu.VMEM((2 * nao, width), jnp.bfloat16),
            pltpu.VMEM((2 * funcs, nao, width), jnp.bfloat16),
            pltpu.VMEM((2 * funcs, 2 * rows, width), jnp.bfloat16),
            pltpu.VMEM((2, rows, nao), jnp.float32),
            pltpu.SemaphoreType.DMA((2 * funcs,)),
            pltpu.SemaphoreType.DMA,
            pltpu.SemaphoreType.DMA,
        ],
        input_output_aliases=aliases,
        compiler_params=pltpu.CompilerParams(vmem_limit_bytes=VMEM_LIMIT),
        cost_estimate=pl.CostEstimate(flops=flops, transcendentals=0, bytes_accessed=6 << 20),
    )(*operands)


def paired_body(pair_tensors, orbitals, matchings):
    per_device, nao, width = orbitals.shape
    rows = nao // lax.axis_size("aux")
    blocks = lax.axis_size("kpt")
    factor = 1.0 / (ROUNDS * pair_tensors.shape[2] * lax.axis_size("aux") * (width // 2)) ** 0.5
    offset = lax.axis_index("kpt") * per_device
    piece = lax.dynamic_slice_in_dim(orbitals, lax.axis_index("aux") * rows, rows, 1)
    within = lax.dynamic_slice_in_dim(matchings, offset, per_device, 1) % per_device
    spots = jnp.arange(per_device, dtype=jnp.int32)
    hits = within[:, None, :] == spots[None, :, None]
    users = jnp.sum(jnp.where(hits, spots[None, None, :], 0), axis=2, dtype=jnp.int32)
    arrived = []
    sibling = from_sibling(pair_tensors)
    for wave in range(ROUNDS):
        targets = wave_targets(blocks, wave)
        for start in range(per_device):
            arrived.append((wave, start, lax.ppermute(piece[start : start + 1], "kpt", targets)))
    running = None
    for wave, start, mine in arrived:
        other = from_sibling(mine)
        running = add_terms(
            users, pair_tensors, sibling, mine, other, running, factor, wave, start, blocks
        )
    return running


def build_block(chosen):
    occupied = chosen.shape[-1] // 2
    real_part = chosen[..., :occupied]
    imag_part = chosen[..., occupied:]
    upper_rows = jnp.concatenate([real_part, imag_part], axis=-1)
    bottom = jnp.concatenate([-imag_part, real_part], axis=-1)
    return jnp.concatenate([upper_rows, bottom], axis=-2)


def half_transform(pairs, block):
    return jnp.einsum("kpab,kbc->kpac", pairs, block, preferred_element_type=jnp.float32).astype(
        jnp.bfloat16
    )


def hermitian_rows(left_rows, half_done):
    occupied = half_done.shape[-1] // 2
    rotated = jnp.concatenate([-half_done[..., occupied:], half_done[..., :occupied]], axis=-1)
    exch_real = jnp.einsum(
        "kpac,kpbc->kab", left_rows, half_done, preferred_element_type=jnp.float32
    )
    exch_imag = jnp.einsum("kpac,kpbc->kab", left_rows, rotated, preferred_element_type=jnp.float32)
    return jnp.stack([exch_real, exch_imag], axis=1)


def wide_body(pair_tensors, orbitals, matchings):
    per_device = orbitals.shape[0]
    occupied = orbitals.shape[2] // 2
    bit_count = lax.axis_size("kpt").bit_length() - 1
    factor = 1.0 / (ROUNDS * pair_tensors.shape[2] * lax.axis_size("aux") * occupied) ** 0.5
    offset = lax.axis_index("kpt") * per_device
    stride = orbitals.shape[2] // lax.axis_size("aux")
    piece = lax.dynamic_slice_in_dim(orbitals, lax.axis_index("aux") * stride, stride, 2)
    collected = []
    for which_round in range(ROUNDS):
        arrived = from_partner(piece, "kpt", bit_count - 1 - which_round)
        partner = lax.all_gather(arrived, "aux", axis=2, tiled=True)
        within = lax.dynamic_slice_in_dim(matchings[which_round], offset, per_device) % per_device
        chosen = jnp.take(partner, within, axis=0)
        half_done = half_transform(pair_tensors[which_round], build_block(chosen))
        collected.append(hermitian_rows(half_done, half_done) * factor)
    return lax.psum_scatter(sum(collected), "aux", scatter_dimension=2, tiled=True)


def body(pair_tensors, orbitals, matchings):
    if lax.axis_size("aux") == 2 and lax.axis_size("kpt") % 4 == 0:
        return paired_body(pair_tensors, orbitals, matchings)
    return wide_body(pair_tensors, orbitals, matchings)


def solution(mesh):
    placed = (P(None, "kpt", "aux", None, None), P("kpt", None, None), P())
    return jax.shard_map(
        body, mesh=mesh, in_specs=placed, out_specs=P("kpt", None, "aux", None), check_vma=False
    )
```

```python
import functools

import jax
import jax.numpy as jnp
from jax import lax
from jax.experimental import pallas as pl
from jax.experimental.pallas import tpu as pltpu
from jax.sharding import PartitionSpec as P


ROUNDS = 2
PARTS = 2
VMEM_LIMIT = 12 << 20
STAGE_LIMIT = 55 << 20
SMEM = pl.BlockSpec(memory_space=pltpu.SMEM)
VMEM = pl.BlockSpec(memory_space=pltpu.VMEM)
HBM = pl.BlockSpec(memory_space=pltpu.HBM)


def from_partner(shard, axis, distance):
    return lax.ppermute(shard, axis, [(i, i ^ 1 << distance) for i in range(lax.axis_size(axis))])


def from_sibling(shard):
    return lax.ppermute(shard, "aux", [(0, 1), (1, 0)])


def hop_round(index, blocks, wave):
    top = index // (blocks // 4)
    return (top + top // 2 + wave + 1) % 2


def wave_targets(blocks, wave):
    bit_count = blocks.bit_length() - 1
    pairs = []
    for index in range(blocks):
        for which_round in range(ROUNDS):
            partner = index ^ 1 << (bit_count - 1 - which_round)
            if hop_round(partner, blocks, wave) == which_round:
                pairs.append((index, partner))
    return pairs


def stage_kernel(users, pair_ref, *rest, blocks):
    out_refs, slot_ref, sems = rest[:ROUNDS], rest[ROUNDS], rest[-1]
    core = lax.axis_index("aux")
    index = lax.axis_index("kpt")
    loads = []
    for wave, out_ref in enumerate(out_refs):
        source = pair_ref.at[hop_round(index, blocks, wave), users[wave, core]]
        loads.append(pltpu.make_async_copy(source, out_ref, sems.at[wave]))
        loads[-1].start()
    for side, at in enumerate((core, 1 - core)):
        slot_ref[side] = jnp.full(slot_ref.shape[1:], users[ROUNDS - 1, at], jnp.int32)
    for load in loads:
        load.wait()


def stage(users, pair_tensors, blocks):
    shape = jax.ShapeDtypeStruct(pair_tensors.shape[2:], pair_tensors.dtype)
    slots = jax.ShapeDtypeStruct((2, 8, 128), jnp.int32)
    return pl.pallas_call(
        functools.partial(stage_kernel, blocks=blocks),
        out_shape=(shape,) * ROUNDS + (slots,),
        in_specs=[SMEM, HBM],
        out_specs=(VMEM,) * (ROUNDS + 1),
        scratch_shapes=[pltpu.SemaphoreType.DMA((ROUNDS,))],
        compiler_params=pltpu.CompilerParams(vmem_limit_bytes=STAGE_LIMIT),
        name="stage",
    )(users, pair_tensors)


def term_kernel(*rest, factor, wave, part, fetch, earlier, blocks):
    users = None
    if not (wave and part):
        users, *rest = rest
    own_ref, sib_ref, mine_ref, *rest = rest
    sources, rest = rest[:earlier], rest[earlier:]
    if fetch is not None:
        full_ref, out_ref, got_ref, block_ref, left_ref, sem = (sib_ref, *rest)
        if part:
            full_ref, sources = sources[-1], sources[:-1]
    elif wave and part:
        out_ref, send_ref, block_ref, left_ref = rest
    else:
        out_ref, block_ref, left_ref = rest
    nao, width = mine_ref.shape
    funcs = own_ref.shape[0]
    occupied = width // 2
    core = lax.axis_index("aux")
    if fetch is not None:
        which_round = hop_round(lax.axis_index("kpt"), blocks, fetch)
        load = pltpu.make_async_copy(full_ref.at[which_round, users[fetch, core]], got_ref, sem)
        load.start()
    block_ref[:nao, :] = mine_ref[...]
    block_ref[nao:, :occupied] = -mine_ref[:, occupied:]
    block_ref[nao:, occupied:] = mine_ref[:, :occupied]
    for q in range(2 * funcs):
        if q < funcs:
            pair = own_ref[q]
        elif fetch == wave:
            if q == funcs:
                load.wait()
            pair = got_ref[q - funcs]
        else:
            pair = sib_ref[q - funcs]
        half = jnp.dot(pair, block_ref[...], preferred_element_type=jnp.float32)
        half = half.astype(jnp.bfloat16)
        at = q * width
        left_ref[0, :, at : at + width] = half
        left_ref[1, :, at : at + occupied] = half[:, occupied:]
        left_ref[1, :, at + occupied : at + width] = -half[:, :occupied]
    if len(sources) == 2:
        same = users[wave - 1, core] == users[wave, core]
    for kind in range(2):
        total = lax.dot_general(
            left_ref[kind], left_ref[0], (((1,), (1,)), ((), ())), preferred_element_type=jnp.float32
        )
        total = total * factor
        if len(sources) == 1:
            total = sources[0][kind] + total
        if len(sources) == 2:
            total = jnp.where(same, sources[0][kind], sources[1][kind]) + total
        if wave and part:
            rows = out_ref.shape[1]
            flip = core == 0
            out_ref[kind] = jnp.where(flip, total[:rows], total[rows:])
            send_ref[kind] = jnp.where(flip, total[rows:], total[:rows])
        else:
            out_ref[kind] = total
    if fetch is not None and fetch != wave:
        load.wait()


def add_terms(users, own, sib, mine, sources, full, factor, wave, part, blocks):
    nao, width = mine.shape
    funcs = own.shape[0]
    whole = jax.ShapeDtypeStruct((2, nao, nao), jnp.float32)
    rows_shape = jax.ShapeDtypeStruct((2, nao // 2, nao), jnp.float32)
    pair_shape = jax.ShapeDtypeStruct(own.shape, own.dtype)
    fetch = {(0, 0): 0, (0, 1): 1}.get((wave, part))
    scratch = [
        pltpu.VMEM((2 * nao, width), jnp.bfloat16),
        pltpu.VMEM((2, nao, 2 * funcs * width), jnp.bfloat16),
    ]
    if fetch is None:
        out_shape = (rows_shape, rows_shape) if part else (whole,)
    else:
        out_shape = (whole, pair_shape)
        scratch.append(pltpu.SemaphoreType.DMA)
    operands = [users, own, full if fetch == 0 else sib, mine, *sources]
    in_specs = [SMEM, VMEM, HBM if fetch == 0 else VMEM, VMEM] + [VMEM] * len(sources)
    if fetch == 1:
        operands.append(full)
        in_specs.append(HBM)
    flops = funcs * 2 * (2 * nao * 2 * nao * width + 2 * 2 * nao * nao * width)
    kernel = functools.partial(
        term_kernel,
        factor=factor,
        wave=wave,
        part=part,
        fetch=fetch,
        earlier=len(operands) - 4,
        blocks=blocks,
    )
    if fetch is None and part:
        operands, in_specs = operands[1:], in_specs[1:]
    return pl.pallas_call(
        kernel,
        out_shape=out_shape,
        in_specs=in_specs,
        out_specs=(VMEM,) * len(out_shape),
        scratch_shapes=scratch,
        compiler_params=pltpu.CompilerParams(vmem_limit_bytes=VMEM_LIMIT),
        cost_estimate=pl.CostEstimate(flops=flops, transcendentals=0, bytes_accessed=6 << 20),
    )(*operands)


def place_kernel(slot_ref, got_ref, *rest, side):
    out_ref, sem = rest[-2:]
    spot = jnp.max(slot_ref[side])
    store = pltpu.make_async_copy(got_ref, out_ref.at[spot], sem)
    store.start()
    store.wait()


def place(slots, got, partial_out, per_device):
    operands = [slots, got]
    in_specs = [VMEM, VMEM]
    aliases = {}
    if partial_out is not None:
        operands.append(partial_out)
        in_specs.append(HBM)
        aliases = {2: 0}
    return pl.pallas_call(
        functools.partial(place_kernel, side=len(aliases)),
        out_shape=jax.ShapeDtypeStruct((per_device,) + got.shape, got.dtype),
        in_specs=in_specs,
        out_specs=HBM,
        scratch_shapes=[pltpu.SemaphoreType.DMA],
        input_output_aliases=aliases,
        compiler_params=pltpu.CompilerParams(vmem_limit_bytes=VMEM_LIMIT),
        name="place",
    )(*operands)


def paired_body(pair_tensors, orbitals, matchings):
    per_device, _, width = orbitals.shape
    occupied = width // 2
    blocks = lax.axis_size("kpt")
    factor = 1.0 / (ROUNDS * pair_tensors.shape[2] * lax.axis_size("aux") * occupied) ** 0.5
    offset = lax.axis_index("kpt") * per_device
    share = occupied // PARTS
    piece = lax.dynamic_index_in_dim(orbitals, lax.axis_index("aux"), 0, keepdims=False)
    sib = from_sibling(pair_tensors)
    arrived = []
    for wave in range(ROUNDS):
        targets = wave_targets(blocks, wave)
        for part in range(PARTS):
            real_part = piece[:, part * share : (part + 1) * share]
            imag_part = piece[:, occupied + part * share : occupied + (part + 1) * share]
            chunk = jnp.concatenate([real_part, imag_part], axis=1)
            arrived.append((wave, part, lax.ppermute(chunk, "kpt", targets)))
    within = lax.dynamic_slice_in_dim(matchings, offset, per_device, 1) % per_device
    spots = jnp.arange(per_device, dtype=jnp.int32)
    hits = within[:, None, :] == spots[None, :, None]
    users = jnp.sum(jnp.where(hits, spots[None, None, :], 0), axis=2, dtype=jnp.int32)
    first_round = hop_round(lax.axis_index("kpt"), blocks, 0)
    users = jnp.where(first_round == 0, users, users[::-1])
    *own, slots = stage(users, pair_tensors, blocks)
    sources = []
    near = None
    for wave, part, mine in arrived:
        got = add_terms(users, own[wave], near, mine, sources, sib, factor, wave, part, blocks)
        if wave == 0 and part == 0:
            near = got[1]
        sources = [got[0]]
        if wave == 0 and part == PARTS - 1:
            near = got[1]
            sources = [got[0], from_sibling(got[0])]
    received = from_sibling(got[1])
    kept = place(slots, got[0], None, per_device)
    return place(slots, received, kept, per_device)


def build_block(chosen):
    occupied = chosen.shape[-1] // 2
    real_part = chosen[..., :occupied]
    imag_part = chosen[..., occupied:]
    upper_rows = jnp.concatenate([real_part, imag_part], axis=-1)
    bottom = jnp.concatenate([-imag_part, real_part], axis=-1)
    return jnp.concatenate([upper_rows, bottom], axis=-2)


def half_transform(pairs, block):
    return jnp.einsum("kpab,kbc->kpac", pairs, block, preferred_element_type=jnp.float32).astype(
        jnp.bfloat16
    )


def hermitian_rows(left_rows, half_done):
    occupied = half_done.shape[-1] // 2
    rotated = jnp.concatenate([-half_done[..., occupied:], half_done[..., :occupied]], axis=-1)
    exch_real = jnp.einsum(
        "kpac,kpbc->kab", left_rows, half_done, preferred_element_type=jnp.float32
    )
    exch_imag = jnp.einsum("kpac,kpbc->kab", left_rows, rotated, preferred_element_type=jnp.float32)
    return jnp.stack([exch_real, exch_imag], axis=1)


def wide_body(pair_tensors, orbitals, matchings):
    per_device = orbitals.shape[0]
    occupied = orbitals.shape[2] // 2
    bit_count = lax.axis_size("kpt").bit_length() - 1
    factor = 1.0 / (ROUNDS * pair_tensors.shape[2] * lax.axis_size("aux") * occupied) ** 0.5
    offset = lax.axis_index("kpt") * per_device
    stride = orbitals.shape[2] // lax.axis_size("aux")
    piece = lax.dynamic_slice_in_dim(orbitals, lax.axis_index("aux") * stride, stride, 2)
    collected = []
    for which_round in range(ROUNDS):
        arrived = from_partner(piece, "kpt", bit_count - 1 - which_round)
        partner = lax.all_gather(arrived, "aux", axis=2, tiled=True)
        within = lax.dynamic_slice_in_dim(matchings[which_round], offset, per_device) % per_device
        chosen = jnp.take(partner, within, axis=0)
        half_done = half_transform(pair_tensors[which_round], build_block(chosen))
        collected.append(hermitian_rows(half_done, half_done) * factor)
    return lax.psum_scatter(sum(collected), "aux", scatter_dimension=2, tiled=True)


def body(pair_tensors, orbitals, matchings):
    shares = orbitals.shape[0]
    if lax.axis_size("aux") == shares == 2 and lax.axis_size("kpt") % 4 == 0:
        return paired_body(pair_tensors, orbitals, matchings)
    return wide_body(pair_tensors, orbitals, matchings)


def solution(mesh):
    placed = (P(None, "kpt", "aux", None, None), P("kpt", None, None), P())
    return jax.shard_map(
        body, mesh=mesh, in_specs=placed, out_specs=P("kpt", None, "aux", None), check_vma=False
    )
```

```python
import functools

import jax
import jax.numpy as jnp
from jax import lax
from jax.experimental import pallas as pl
from jax.experimental.pallas import tpu as pltpu
from jax.sharding import PartitionSpec as P


ROUNDS = 2
PARTS = 2
VMEM_LIMIT = 12 << 20
STAGE_LIMIT = 44 << 20
SMEM = pl.BlockSpec(memory_space=pltpu.SMEM)
VMEM = pl.BlockSpec(memory_space=pltpu.VMEM)
HBM = pl.BlockSpec(memory_space=pltpu.HBM)


def from_partner(shard, axis, distance):
    return lax.ppermute(shard, axis, [(i, i ^ 1 << distance) for i in range(lax.axis_size(axis))])


def from_sibling(shard):
    return lax.ppermute(shard, "aux", [(0, 1), (1, 0)])


def hop_round(index, blocks, wave):
    top = index // (blocks // 4)
    return (top + top // 2 + wave + 1) % 2


def wave_targets(blocks, wave):
    bit_count = blocks.bit_length() - 1
    pairs = []
    for index in range(blocks):
        for which_round in range(ROUNDS):
            partner = index ^ 1 << (bit_count - 1 - which_round)
            if hop_round(partner, blocks, wave) == which_round:
                pairs.append((index, partner))
    return pairs


def stage_kernel(users, pair_ref, *rest, blocks):
    out_refs, slot_ref, sems = rest[:ROUNDS], rest[ROUNDS], rest[-1]
    core = lax.axis_index("aux")
    index = lax.axis_index("kpt")
    loads = []
    for wave, out_ref in enumerate(out_refs):
        source = pair_ref.at[hop_round(index, blocks, wave), users[wave, core]]
        loads.append(pltpu.make_async_copy(source, out_ref, sems.at[wave]))
        loads[-1].start()
    for side, at in enumerate((core, 1 - core)):
        slot_ref[side] = jnp.full(slot_ref.shape[1:], users[ROUNDS - 1, at], jnp.int32)
    for load in loads:
        load.wait()


def stage(users, pair_tensors, blocks):
    shape = jax.ShapeDtypeStruct(pair_tensors.shape[2:], pair_tensors.dtype)
    slots = jax.ShapeDtypeStruct((2, 8, 128), jnp.int32)
    return pl.pallas_call(
        functools.partial(stage_kernel, blocks=blocks),
        out_shape=(shape,) * ROUNDS + (slots,),
        in_specs=[SMEM, HBM],
        out_specs=(VMEM,) * (ROUNDS + 1),
        scratch_shapes=[pltpu.SemaphoreType.DMA((ROUNDS,))],
        compiler_params=pltpu.CompilerParams(vmem_limit_bytes=STAGE_LIMIT),
        name="stage",
    )(users, pair_tensors)


def hand_out(total, keep_ref, send_ref):
    rows = keep_ref.shape[0]
    flip = lax.axis_index("aux") == 0
    keep_ref[...] = jnp.where(flip, total[:rows], total[rows:])
    send_ref[...] = jnp.where(flip, total[rows:], total[:rows])


def imag_kernel(left_ref, source_ref, keep_ref, send_ref, *, factor):
    total = lax.dot_general(
        left_ref[1], left_ref[0], (((1,), (1,)), ((), ())), preferred_element_type=jnp.float32
    )
    hand_out(source_ref[1] + total * factor, keep_ref, send_ref)


def add_imag(left, source, factor):
    nao = left.shape[1]
    rows_shape = jax.ShapeDtypeStruct((nao // 2, nao), jnp.float32)
    return pl.pallas_call(
        functools.partial(imag_kernel, factor=factor),
        out_shape=(rows_shape,) * 2,
        in_specs=[VMEM] * 2,
        out_specs=(VMEM,) * 2,
        compiler_params=pltpu.CompilerParams(vmem_limit_bytes=VMEM_LIMIT),
        cost_estimate=pl.CostEstimate(
            flops=2 * nao * nao * left.shape[2], transcendentals=0, bytes_accessed=2 << 20
        ),
        name="add_imag",
    )(left, source)


def term_kernel(*rest, factor, wave, part, fetch, earlier, blocks):
    users = None
    if not (wave and part):
        users, *rest = rest
    own_ref, sib_ref, mine_ref, *rest = rest
    sources, rest = rest[:earlier], rest[earlier:]
    if fetch is not None:
        full_ref, out_ref, got_ref, block_ref, left_ref, sem = (sib_ref, *rest)
        if part:
            full_ref, sources = sources[-1], sources[:-1]
    elif wave and part:
        out_ref, send_ref, left_ref, block_ref = rest
    else:
        out_ref, block_ref, left_ref = rest
    nao, width = mine_ref.shape
    funcs = own_ref.shape[0]
    occupied = width // 2
    core = lax.axis_index("aux")
    if fetch is not None:
        which_round = hop_round(lax.axis_index("kpt"), blocks, fetch)
        load = pltpu.make_async_copy(full_ref.at[which_round, users[fetch, core]], got_ref, sem)
        load.start()
    block_ref[:nao, :] = mine_ref[...]
    block_ref[nao:, :occupied] = -mine_ref[:, occupied:]
    block_ref[nao:, occupied:] = mine_ref[:, :occupied]
    for q in range(2 * funcs):
        if q < funcs:
            pair = own_ref[q]
        elif fetch == wave:
            if q == funcs:
                load.wait()
            pair = got_ref[q - funcs]
        else:
            pair = sib_ref[q - funcs]
        half = jnp.dot(pair, block_ref[...], preferred_element_type=jnp.float32)
        half = half.astype(jnp.bfloat16)
        at = q * width
        left_ref[0, :, at : at + width] = half
        left_ref[1, :, at : at + occupied] = half[:, occupied:]
        left_ref[1, :, at + occupied : at + width] = -half[:, :occupied]
    if len(sources) == 2:
        same = users[wave - 1, core] == users[wave, core]
    for kind in range(1 if wave and part else 2):
        total = lax.dot_general(
            left_ref[kind], left_ref[0], (((1,), (1,)), ((), ())), preferred_element_type=jnp.float32
        )
        total = total * factor
        if len(sources) == 1:
            total = sources[0][kind] + total
        if len(sources) == 2:
            total = jnp.where(same, sources[0][kind], sources[1][kind]) + total
        if wave and part:
            hand_out(total, out_ref, send_ref)
        else:
            out_ref[kind] = total
    if fetch is not None and fetch != wave:
        load.wait()


def add_terms(users, own, sib, mine, sources, full, factor, wave, part, blocks):
    nao, width = mine.shape
    funcs = own.shape[0]
    whole = jax.ShapeDtypeStruct((2, nao, nao), jnp.float32)
    rows_shape = jax.ShapeDtypeStruct((nao // 2, nao), jnp.float32)
    pair_shape = jax.ShapeDtypeStruct(own.shape, own.dtype)
    fetch = {(0, 0): 0, (0, 1): 1}.get((wave, part))
    scratch = [
        pltpu.VMEM((2 * nao, width), jnp.bfloat16),
        pltpu.VMEM((2, nao, 2 * funcs * width), jnp.bfloat16),
    ]
    if fetch is None:
        out_shape = (whole,)
        if part:
            left_shape = jax.ShapeDtypeStruct((2, nao, 2 * funcs * width), jnp.bfloat16)
            out_shape = (rows_shape, rows_shape, left_shape)
            scratch.pop()
    else:
        out_shape = (whole, pair_shape)
        scratch.append(pltpu.SemaphoreType.DMA)
    operands = [users, own, full if fetch == 0 else sib, mine, *sources]
    in_specs = [SMEM, VMEM, HBM if fetch == 0 else VMEM, VMEM] + [VMEM] * len(sources)
    if fetch == 1:
        operands.append(full)
        in_specs.append(HBM)
    flops = funcs * 2 * (2 * nao * 2 * nao * width + 2 * 2 * nao * nao * width)
    kernel = functools.partial(
        term_kernel,
        factor=factor,
        wave=wave,
        part=part,
        fetch=fetch,
        earlier=len(operands) - 4,
        blocks=blocks,
    )
    if fetch is None and part:
        operands, in_specs = operands[1:], in_specs[1:]
    return pl.pallas_call(
        kernel,
        out_shape=out_shape,
        in_specs=in_specs,
        out_specs=(VMEM,) * len(out_shape),
        scratch_shapes=scratch,
        compiler_params=pltpu.CompilerParams(vmem_limit_bytes=VMEM_LIMIT),
        cost_estimate=pl.CostEstimate(flops=flops, transcendentals=0, bytes_accessed=6 << 20),
    )(*operands)


def place_kernel(slot_ref, real_ref, imag_ref, *rest, side):
    out_ref, sems = rest[-2:]
    spot = jnp.max(slot_ref[side])
    stores = []
    for kind, got_ref in enumerate((real_ref, imag_ref)):
        stores.append(pltpu.make_async_copy(got_ref, out_ref.at[spot, kind], sems.at[kind]))
        stores[-1].start()
    for store in stores:
        store.wait()


def place(slots, got, partial_out, per_device):
    operands = [slots, *got]
    in_specs = [VMEM] * 3
    aliases = {}
    if partial_out is not None:
        operands.append(partial_out)
        in_specs.append(HBM)
        aliases = {3: 0}
    return pl.pallas_call(
        functools.partial(place_kernel, side=len(aliases)),
        out_shape=jax.ShapeDtypeStruct((per_device, 2) + got[0].shape, jnp.float32),
        in_specs=in_specs,
        out_specs=HBM,
        scratch_shapes=[pltpu.SemaphoreType.DMA((2,))],
        input_output_aliases=aliases,
        compiler_params=pltpu.CompilerParams(vmem_limit_bytes=VMEM_LIMIT),
        name="place",
    )(*operands)


def paired_body(pair_tensors, orbitals, matchings):
    per_device, _, width = orbitals.shape
    occupied = width // 2
    blocks = lax.axis_size("kpt")
    factor = 1.0 / (ROUNDS * pair_tensors.shape[2] * lax.axis_size("aux") * occupied) ** 0.5
    offset = lax.axis_index("kpt") * per_device
    share = occupied // PARTS
    piece = lax.dynamic_index_in_dim(orbitals, lax.axis_index("aux"), 0, keepdims=False)
    sib = from_sibling(pair_tensors)
    arrived = []
    for wave in range(ROUNDS):
        targets = wave_targets(blocks, wave)
        for part in range(PARTS):
            real_part = piece[:, part * share : (part + 1) * share]
            imag_part = piece[:, occupied + part * share : occupied + (part + 1) * share]
            chunk = jnp.concatenate([real_part, imag_part], axis=1)
            arrived.append((wave, part, lax.ppermute(chunk, "kpt", targets)))
    within = lax.dynamic_slice_in_dim(matchings, offset, per_device, 1) % per_device
    spots = jnp.arange(per_device, dtype=jnp.int32)
    hits = within[:, None, :] == spots[None, :, None]
    users = jnp.sum(jnp.where(hits, spots[None, None, :], 0), axis=2, dtype=jnp.int32)
    first_round = hop_round(lax.axis_index("kpt"), blocks, 0)
    users = jnp.where(first_round == 0, users, users[::-1])
    *own, slots = stage(users, pair_tensors, blocks)
    sources = []
    near = None
    for wave, part, mine in arrived:
        before = sources[0] if sources else None
        got = add_terms(users, own[wave], near, mine, sources, sib, factor, wave, part, blocks)
        if wave == 0 and part == 0:
            near = got[1]
        sources = [got[0]]
        if wave == 0 and part == PARTS - 1:
            near = got[1]
            sources = [got[0], from_sibling(got[0])]
    keep_real, send_real, left = got
    real = from_sibling(send_real)
    keep_imag, send_imag = add_imag(left, before, factor)
    imag = from_sibling(send_imag)
    kept = place(slots, (keep_real, keep_imag), None, per_device)
    return place(slots, (real, imag), kept, per_device)


def build_block(chosen):
    occupied = chosen.shape[-1] // 2
    real_part = chosen[..., :occupied]
    imag_part = chosen[..., occupied:]
    upper_rows = jnp.concatenate([real_part, imag_part], axis=-1)
    bottom = jnp.concatenate([-imag_part, real_part], axis=-1)
    return jnp.concatenate([upper_rows, bottom], axis=-2)


def half_transform(pairs, block):
    return jnp.einsum("kpab,kbc->kpac", pairs, block, preferred_element_type=jnp.float32).astype(
        jnp.bfloat16
    )


def hermitian_rows(left_rows, half_done):
    occupied = half_done.shape[-1] // 2
    rotated = jnp.concatenate([-half_done[..., occupied:], half_done[..., :occupied]], axis=-1)
    exch_real = jnp.einsum(
        "kpac,kpbc->kab", left_rows, half_done, preferred_element_type=jnp.float32
    )
    exch_imag = jnp.einsum("kpac,kpbc->kab", left_rows, rotated, preferred_element_type=jnp.float32)
    return jnp.stack([exch_real, exch_imag], axis=1)


def wide_body(pair_tensors, orbitals, matchings):
    per_device = orbitals.shape[0]
    occupied = orbitals.shape[2] // 2
    bit_count = lax.axis_size("kpt").bit_length() - 1
    factor = 1.0 / (ROUNDS * pair_tensors.shape[2] * lax.axis_size("aux") * occupied) ** 0.5
    offset = lax.axis_index("kpt") * per_device
    stride = orbitals.shape[2] // lax.axis_size("aux")
    piece = lax.dynamic_slice_in_dim(orbitals, lax.axis_index("aux") * stride, stride, 2)
    collected = []
    for which_round in range(ROUNDS):
        arrived = from_partner(piece, "kpt", bit_count - 1 - which_round)
        partner = lax.all_gather(arrived, "aux", axis=2, tiled=True)
        within = lax.dynamic_slice_in_dim(matchings[which_round], offset, per_device) % per_device
        chosen = jnp.take(partner, within, axis=0)
        half_done = half_transform(pair_tensors[which_round], build_block(chosen))
        collected.append(hermitian_rows(half_done, half_done) * factor)
    return lax.psum_scatter(sum(collected), "aux", scatter_dimension=2, tiled=True)


def body(pair_tensors, orbitals, matchings):
    shares = orbitals.shape[0]
    if lax.axis_size("aux") == shares == 2 and lax.axis_size("kpt") % 4 == 0:
        return paired_body(pair_tensors, orbitals, matchings)
    return wide_body(pair_tensors, orbitals, matchings)


def solution(mesh):
    placed = (P(None, "kpt", "aux", None, None), P("kpt", None, None), P())
    return jax.shard_map(
        body, mesh=mesh, in_specs=placed, out_specs=P("kpt", None, "aux", None), check_vma=False
    )
```

```python
import functools

import jax
import jax.numpy as jnp
from jax import lax
from jax.experimental import pallas as pl
from jax.experimental.pallas import tpu as pltpu
from jax.sharding import PartitionSpec as P


ROUNDS = 2
PARTS = ((2, 2), (2, 1, 1))
VMEM_LIMIT = 12 << 20
STAGE_LIMIT = 44 << 20
SMEM = pl.BlockSpec(memory_space=pltpu.SMEM)
VMEM = pl.BlockSpec(memory_space=pltpu.VMEM)
HBM = pl.BlockSpec(memory_space=pltpu.HBM)


def from_partner(shard, axis, distance):
    return lax.ppermute(shard, axis, [(i, i ^ 1 << distance) for i in range(lax.axis_size(axis))])


def from_sibling(shard):
    return lax.ppermute(shard, "aux", [(0, 1), (1, 0)])


def hop_round(index, blocks, wave):
    top = index // (blocks // 4)
    return (top + top // 2 + wave + 1) % 2


def wave_targets(blocks, wave):
    bit_count = blocks.bit_length() - 1
    pairs = []
    for index in range(blocks):
        for which_round in range(ROUNDS):
            partner = index ^ 1 << (bit_count - 1 - which_round)
            if hop_round(partner, blocks, wave) == which_round:
                pairs.append((index, partner))
    return pairs


def stage_kernel(users, pair_ref, *rest, blocks):
    out_refs, slot_ref, sems = rest[:ROUNDS], rest[ROUNDS], rest[-1]
    core = lax.axis_index("aux")
    index = lax.axis_index("kpt")
    loads = []
    for wave, out_ref in enumerate(out_refs):
        source = pair_ref.at[hop_round(index, blocks, wave), users[wave, core]]
        loads.append(pltpu.make_async_copy(source, out_ref, sems.at[wave]))
        loads[-1].start()
    for side, at in enumerate((core, 1 - core)):
        slot_ref[side] = jnp.full(slot_ref.shape[1:], users[ROUNDS - 1, at], jnp.int32)
    same = (users[0, core] == users[ROUNDS - 1, core]).astype(jnp.int32)
    slot_ref[2] = jnp.full(slot_ref.shape[1:], same, jnp.int32)
    for load in loads:
        load.wait()


def stage(users, pair_tensors, blocks):
    shape = jax.ShapeDtypeStruct(pair_tensors.shape[2:], pair_tensors.dtype)
    slots = jax.ShapeDtypeStruct((3, 8, 128), jnp.int32)
    return pl.pallas_call(
        functools.partial(stage_kernel, blocks=blocks),
        out_shape=(shape,) * ROUNDS + (slots,),
        in_specs=[SMEM, HBM],
        out_specs=(VMEM,) * (ROUNDS + 1),
        scratch_shapes=[pltpu.SemaphoreType.DMA((ROUNDS,))],
        compiler_params=pltpu.CompilerParams(vmem_limit_bytes=STAGE_LIMIT),
        name="stage",
    )(users, pair_tensors)


def hand_out(total, keep_ref, send_ref):
    rows = keep_ref.shape[0]
    flip = lax.axis_index("aux") == 0
    keep_ref[...] = jnp.where(flip, total[:rows], total[rows:])
    send_ref[...] = jnp.where(flip, total[rows:], total[:rows])


def imag_kernel(left_ref, source_ref, keep_ref, send_ref, *, factor):
    total = lax.dot_general(
        left_ref[1], left_ref[0], (((1,), (1,)), ((), ())), preferred_element_type=jnp.float32
    )
    hand_out(source_ref[1] + total * factor, keep_ref, send_ref)


def fold_kernel(slot_ref, sums_ref, own_ref, other_ref, out_ref):
    same = jnp.max(slot_ref[2]) > 0
    out_ref[...] = sums_ref[...] + jnp.where(same, own_ref[...], other_ref[...])


def fold(slots, sums, own, other):
    return pl.pallas_call(
        fold_kernel,
        out_shape=jax.ShapeDtypeStruct(sums.shape, sums.dtype),
        in_specs=[VMEM] * 4,
        out_specs=VMEM,
        compiler_params=pltpu.CompilerParams(vmem_limit_bytes=VMEM_LIMIT),
        name="fold",
    )(slots, sums, own, other)


def add_imag(left, source, factor):
    nao = left.shape[1]
    rows_shape = jax.ShapeDtypeStruct((nao // 2, nao), jnp.float32)
    return pl.pallas_call(
        functools.partial(imag_kernel, factor=factor),
        out_shape=(rows_shape,) * 2,
        in_specs=[VMEM] * 2,
        out_specs=(VMEM,) * 2,
        compiler_params=pltpu.CompilerParams(vmem_limit_bytes=VMEM_LIMIT),
        cost_estimate=pl.CostEstimate(
            flops=2 * nao * nao * left.shape[2], transcendentals=0, bytes_accessed=2 << 20
        ),
        name="add_imag",
    )(left, source)


def term_kernel(*rest, factor, wave, part, last, fetch, earlier, blocks):
    users = None
    if fetch is not None:
        users, *rest = rest
    own_ref, sib_ref, mine_ref, *rest = rest
    sources, rest = rest[:earlier], rest[earlier:]
    if fetch is not None:
        full_ref, out_ref, got_ref, block_ref, left_ref, sem = (sib_ref, *rest)
        if part:
            full_ref, sources = sources[-1], sources[:-1]
    elif last:
        out_ref, send_ref, left_ref, block_ref = rest
    else:
        out_ref, block_ref, left_ref = rest
    nao, width = mine_ref.shape
    funcs = own_ref.shape[0]
    occupied = width // 2
    core = lax.axis_index("aux")
    if fetch is not None:
        which_round = hop_round(lax.axis_index("kpt"), blocks, fetch)
        load = pltpu.make_async_copy(full_ref.at[which_round, users[fetch, core]], got_ref, sem)
        load.start()
    block_ref[:nao, :] = mine_ref[...]
    block_ref[nao:, :occupied] = -mine_ref[:, occupied:]
    block_ref[nao:, occupied:] = mine_ref[:, :occupied]
    for q in range(2 * funcs):
        if q < funcs:
            pair = own_ref[q]
        elif fetch == wave:
            if q == funcs:
                load.wait()
            pair = got_ref[q - funcs]
        else:
            pair = sib_ref[q - funcs]
        half = jnp.dot(pair, block_ref[...], preferred_element_type=jnp.float32)
        half = half.astype(jnp.bfloat16)
        at = q * width
        left_ref[0, :, at : at + width] = half
        left_ref[1, :, at : at + occupied] = half[:, occupied:]
        left_ref[1, :, at + occupied : at + width] = -half[:, :occupied]
    for kind in range(1 if last else 2):
        total = lax.dot_general(
            left_ref[kind], left_ref[0], (((1,), (1,)), ((), ())), preferred_element_type=jnp.float32
        )
        total = total * factor
        if len(sources) == 1:
            total = sources[0][kind] + total
        if last:
            hand_out(total, out_ref, send_ref)
        else:
            out_ref[kind] = total
    if fetch is not None and fetch != wave:
        load.wait()


def add_terms(users, own, sib, mine, sources, full, factor, wave, part, blocks):
    nao, width = mine.shape
    funcs = own.shape[0]
    whole = jax.ShapeDtypeStruct((2, nao, nao), jnp.float32)
    rows_shape = jax.ShapeDtypeStruct((nao // 2, nao), jnp.float32)
    pair_shape = jax.ShapeDtypeStruct(own.shape, own.dtype)
    fetch = {(0, 0): 0, (0, 1): 1}.get((wave, part))
    last = wave == 1 and part == len(PARTS[1]) - 1
    scratch = [
        pltpu.VMEM((2 * nao, width), jnp.bfloat16),
        pltpu.VMEM((2, nao, 2 * funcs * width), jnp.bfloat16),
    ]
    if fetch is None:
        out_shape = (whole,)
        if last:
            left_shape = jax.ShapeDtypeStruct((2, nao, 2 * funcs * width), jnp.bfloat16)
            out_shape = (rows_shape, rows_shape, left_shape)
            scratch.pop()
    else:
        out_shape = (whole, pair_shape)
        scratch.append(pltpu.SemaphoreType.DMA)
    operands = [users, own, full if fetch == 0 else sib, mine, *sources]
    in_specs = [SMEM, VMEM, HBM if fetch == 0 else VMEM, VMEM] + [VMEM] * len(sources)
    if fetch == 1:
        operands.append(full)
        in_specs.append(HBM)
    flops = funcs * 2 * (2 * nao * 2 * nao * width + 2 * 2 * nao * nao * width)
    kernel = functools.partial(
        term_kernel,
        factor=factor,
        wave=wave,
        part=part,
        last=last,
        fetch=fetch,
        earlier=len(operands) - 4,
        blocks=blocks,
    )
    if fetch is None:
        operands, in_specs = operands[1:], in_specs[1:]
    return pl.pallas_call(
        kernel,
        out_shape=out_shape,
        in_specs=in_specs,
        out_specs=(VMEM,) * len(out_shape),
        scratch_shapes=scratch,
        compiler_params=pltpu.CompilerParams(vmem_limit_bytes=VMEM_LIMIT),
        cost_estimate=pl.CostEstimate(flops=flops, transcendentals=0, bytes_accessed=6 << 20),
    )(*operands)


def place_kernel(slot_ref, real_ref, imag_ref, *rest, side):
    out_ref, sems = rest[-2:]
    spot = jnp.max(slot_ref[side])
    stores = []
    for kind, got_ref in enumerate((real_ref, imag_ref)):
        stores.append(pltpu.make_async_copy(got_ref, out_ref.at[spot, kind], sems.at[kind]))
        stores[-1].start()
    for store in stores:
        store.wait()


def place(slots, got, partial_out, per_device):
    operands = [slots, *got]
    in_specs = [VMEM] * 3
    aliases = {}
    if partial_out is not None:
        operands.append(partial_out)
        in_specs.append(HBM)
        aliases = {3: 0}
    return pl.pallas_call(
        functools.partial(place_kernel, side=len(aliases)),
        out_shape=jax.ShapeDtypeStruct((per_device, 2) + got[0].shape, jnp.float32),
        in_specs=in_specs,
        out_specs=HBM,
        scratch_shapes=[pltpu.SemaphoreType.DMA((2,))],
        input_output_aliases=aliases,
        compiler_params=pltpu.CompilerParams(vmem_limit_bytes=VMEM_LIMIT),
        name="place",
    )(*operands)


def paired_body(pair_tensors, orbitals, matchings):
    per_device, _, width = orbitals.shape
    occupied = width // 2
    blocks = lax.axis_size("kpt")
    factor = 1.0 / (ROUNDS * pair_tensors.shape[2] * lax.axis_size("aux") * occupied) ** 0.5
    offset = lax.axis_index("kpt") * per_device
    piece = lax.dynamic_index_in_dim(orbitals, lax.axis_index("aux"), 0, keepdims=False)
    sib = from_sibling(pair_tensors)
    arrived = []
    for wave in range(ROUNDS):
        targets = wave_targets(blocks, wave)
        start = 0
        for part, weight in enumerate(PARTS[wave]):
            stop = start + occupied * weight // sum(PARTS[wave])
            real_part = piece[:, start:stop]
            imag_part = piece[:, occupied + start : occupied + stop]
            start = stop
            chunk = jnp.concatenate([real_part, imag_part], axis=1)
            arrived.append((wave, part, lax.ppermute(chunk, "kpt", targets)))
    within = lax.dynamic_slice_in_dim(matchings, offset, per_device, 1) % per_device
    spots = jnp.arange(per_device, dtype=jnp.int32)
    hits = within[:, None, :] == spots[None, :, None]
    users = jnp.sum(jnp.where(hits, spots[None, None, :], 0), axis=2, dtype=jnp.int32)
    first_round = hop_round(lax.axis_index("kpt"), blocks, 0)
    users = jnp.where(first_round == 0, users, users[::-1])
    *own, slots = stage(users, pair_tensors, blocks)
    sources = []
    near = None
    for wave, part, mine in arrived:
        before = sources[0] if sources else None
        got = add_terms(users, own[wave], near, mine, sources, sib, factor, wave, part, blocks)
        if wave == 0 and part == 0:
            near = got[1]
        sources = [got[0]]
        if wave == 0 and part == len(PARTS[0]) - 1:
            near = got[1]
            first_sums = [got[0], from_sibling(got[0])]
            sources = []
        if wave == 1 and part == len(PARTS[1]) - 2:
            sources = [fold(slots, sources[0], *first_sums)]
    keep_real, send_real, left = got
    real = from_sibling(send_real)
    keep_imag, send_imag = add_imag(left, before, factor)
    imag = from_sibling(send_imag)
    kept = place(slots, (keep_real, keep_imag), None, per_device)
    return place(slots, (real, imag), kept, per_device)


def build_block(chosen):
    occupied = chosen.shape[-1] // 2
    real_part = chosen[..., :occupied]
    imag_part = chosen[..., occupied:]
    upper_rows = jnp.concatenate([real_part, imag_part], axis=-1)
    bottom = jnp.concatenate([-imag_part, real_part], axis=-1)
    return jnp.concatenate([upper_rows, bottom], axis=-2)


def half_transform(pairs, block):
    return jnp.einsum("kpab,kbc->kpac", pairs, block, preferred_element_type=jnp.float32).astype(
        jnp.bfloat16
    )


def hermitian_rows(left_rows, half_done):
    occupied = half_done.shape[-1] // 2
    rotated = jnp.concatenate([-half_done[..., occupied:], half_done[..., :occupied]], axis=-1)
    exch_real = jnp.einsum(
        "kpac,kpbc->kab", left_rows, half_done, preferred_element_type=jnp.float32
    )
    exch_imag = jnp.einsum("kpac,kpbc->kab", left_rows, rotated, preferred_element_type=jnp.float32)
    return jnp.stack([exch_real, exch_imag], axis=1)


def wide_body(pair_tensors, orbitals, matchings):
    per_device = orbitals.shape[0]
    occupied = orbitals.shape[2] // 2
    bit_count = lax.axis_size("kpt").bit_length() - 1
    factor = 1.0 / (ROUNDS * pair_tensors.shape[2] * lax.axis_size("aux") * occupied) ** 0.5
    offset = lax.axis_index("kpt") * per_device
    stride = orbitals.shape[2] // lax.axis_size("aux")
    piece = lax.dynamic_slice_in_dim(orbitals, lax.axis_index("aux") * stride, stride, 2)
    collected = []
    for which_round in range(ROUNDS):
        arrived = from_partner(piece, "kpt", bit_count - 1 - which_round)
        partner = lax.all_gather(arrived, "aux", axis=2, tiled=True)
        within = lax.dynamic_slice_in_dim(matchings[which_round], offset, per_device) % per_device
        chosen = jnp.take(partner, within, axis=0)
        half_done = half_transform(pair_tensors[which_round], build_block(chosen))
        collected.append(hermitian_rows(half_done, half_done) * factor)
    return lax.psum_scatter(sum(collected), "aux", scatter_dimension=2, tiled=True)


def body(pair_tensors, orbitals, matchings):
    shares = orbitals.shape[0]
    if lax.axis_size("aux") == shares == 2 and lax.axis_size("kpt") % 4 == 0:
        return paired_body(pair_tensors, orbitals, matchings)
    return wide_body(pair_tensors, orbitals, matchings)


def solution(mesh):
    placed = (P(None, "kpt", "aux", None, None), P("kpt", None, None), P())
    return jax.shard_map(
        body, mesh=mesh, in_specs=placed, out_specs=P("kpt", None, "aux", None), check_vma=False
    )
```
